32 devices in a mesh: group: 2 (over y), gx: 4 (over x, core), gy: 4 (over z).
Axes of the slice: x: 2, y: 2, z: 4, core: 2. Of those that a mesh axis runs over, the one named last changes fastest.
Arguments:
- pressure: float32 [192, 64, 768], P(('group', 'gx'), 'gy'), parts along dimension 0, may hold values from -6 to 6
- pressure_prev: float32 [192, 64, 768], P(('group', 'gx'), 'gy'), parts along dimension 0, may hold values from -6 to 6
- courant: float32 [192, 64, 768], P(('group', 'gx'), 'gy'), parts along dimension 0, may hold values from 0.05 to 0.3
- nonlinearity: float32 [192, 64, 768], P(('group', 'gx'), 'gy'), parts along dimension 0, may hold values from 0.03 to 0.3
- absorption: float32 [192, 64, 768], P(('group', 'gx'), 'gy'), parts along dimension 0, may hold values from 0.2 to 2
- own_map: int32 [96, 32], P(('group', 'gx'), 'gy'), parts along dimension 0, may hold values from 0 to 16, as said below
- slot_table: int32 [96, 32], P(('group', 'gx'), 'gy'), parts along dimension 0, may hold values from 0 to 511
- displacement: float32 [128, 128, 384], P(('group', 'gx'), 'gy'), parts along dimension 0, may hold values from -6 to 6
- displacement_prev: float32 [128, 128, 384], P(('group', 'gx'), 'gy'), parts along dimension 0, may hold values from -6 to 6
- layer_labels: int32 [128, 128, 384], P(('group', 'gx'), 'gy'), parts along dimension 0, may hold values from 0 to 3
- shear_table: float32 [8], P('group'), parts along dimension 0, may hold values from 0.05 to 0.15
- viscosity_table: float32 [8], P('group'), parts along dimension 0, may hold values from 0.01 to 0.06
Outputs:
- pressure_mid: float32 [192, 64, 768], P(('group', 'gx'), 'gy'), parts along dimension 0
- pressure_new: float32 [192, 64, 768], P(('group', 'gx'), 'gy'), parts along dimension 0
- tissue_force: float32 [128, 128, 384], P(('group', 'gx'), 'gy'), parts along dimension 0
- displacement_mid: float32 [128, 128, 384], P(('group', 'gx'), 'gy'), parts along dimension 0
- displacement_new: float32 [128, 128, 384], P(('group', 'gx'), 'gy'), parts along dimension 0
The draws below stay inside these ranges and needn't reach their ends.
There are 2 independent parts, one for each index of `group`. The reference program is written for one: setup_inputs(seed, part) draws one part's arguments, and reference() takes and returns one part's arrays. A program takes and returns all parts, laid end to end along the dimension named above; each array names one. Nothing has to cross between parts.
Inputs may be any that keep to these rules, and one draw needn't show every extreme that they name: `own_map`: A value below 16 names tissue block (v // 4, v % 4); 16 marks a line outside the focal zone. Among the lines of one device's block of the map, at most 6 name any one tissue block, and exactly 6 do for some block in every draw.
All inputs are finite; a program needn't handle non-finite values.
Results may differ from the reference program's by a relative error of at most 0.0003.
Values sent between devices are 32-bit elements; how exact they have to be, the bound alone decides.
A program may use at most 64 MiB of HBM per device.

```python
import math
import jax
import jax.numpy as jnp
from jax import lax

BZ = 24
CX = 16
NY = 768
RX = 16
RY = 32
LAYERS = 4
TZ = 384
NZ = 96
NX = 64
TX = 64
TY = 128
TROWS = 4
TCOLS = 4
TILES = 16
CAP = 6


def focal_routing(key):
    keys = jax.random.split(jax.random.fold_in(key, 7), 2)
    outside_row = jax.random.randint(keys[0], (), 0, TROWS)
    offsets = jax.random.randint(keys[1], (TILES,), 0, TILES)
    depth = BZ // 2
    across = CX // 2
    line_z = jnp.arange(NZ // 2, dtype=jnp.int32)[:, None]
    line_x = jnp.arange(NX // 2, dtype=jnp.int32)[None, :]
    source_row = line_z // depth
    source_col = line_x // across
    local = line_z % depth * across + line_x % across
    group_index = local // CAP
    source = source_row * TCOLS + source_col
    focal = source_row != outside_row
    target = (offsets[source] + group_index) % TILES
    return jnp.where(focal, target, TILES).astype(jnp.int32)


def draw_own_map(key, part):
    return focal_routing(key)


def plant(array, rng, least, high):
    longest = array.shape.index(max(array.shape))
    spots = []
    for shift in (0, 1):
        where = [jax.random.randint(jax.random.fold_in(rng, axis), (), 0, length) for axis, length in enumerate(array.shape)]
        where[longest] = (where[longest] + shift) % array.shape[longest]
        spots.append(tuple(where))
    return array.at[spots[0]].set(least).at[spots[1]].set(high)


def level_of(own_key, dims, cuts, least, largest):
    loudness, own = 1.0, jax.random.fold_in(own_key, 6)
    for position, blocks in cuts:
        draws = jnp.exp(jax.random.uniform(jax.random.fold_in(own, position), (blocks,), jnp.float32, least / len(cuts), largest / len(cuts)))
        loudness = loudness * jnp.repeat(draws, dims[position] // blocks).reshape([-1 if axis == position else 1 for axis in range(len(dims))])
    return loudness


def scatter_about(own_key, shape, deviation, most, cuts=(), kind=jnp.bfloat16):
    entries = deviation * jax.random.normal(own_key, shape, jnp.float32)
    if cuts:
        entries = entries * level_of(own_key, shape, cuts, -0.22, 0.18)
    return jnp.clip(entries, -most, most).astype(kind)


def setup_inputs(seed: int = 0, part: int = 0) -> dict:
    key_of = jax.random.split(jax.random.key(seed), 13)
    part_keys = jax.random.split(jax.random.fold_in(key_of[12], part), 13)
    pressure = scatter_about(part_keys[0], (NZ, NX, NY), 1.0, 6.0, ((0, 4), (1, 4)), jnp.float32)
    pressure_prev = scatter_about(part_keys[1], (NZ, NX, NY), 1.0, 6.0, ((0, 4), (1, 4)), jnp.float32)
    courant = jnp.clip(jnp.exp(math.log(0.3) - 1.7917595 * jax.random.uniform(part_keys[2], (NZ, NX, NY), jnp.float32) ** level_of(part_keys[2], (NZ, NX, NY), ((0, 4), (1, 4)), -0.2, 0.2)), 0.05, 0.3)
    nonlinearity = jnp.clip(jnp.exp(math.log(0.3) - 2.3025852 * jax.random.uniform(part_keys[3], (NZ, NX, NY), jnp.float32) ** level_of(part_keys[3], (NZ, NX, NY), ((0, 4), (1, 4)), -0.2, 0.2)), 0.03, 0.3)
    absorption = jnp.clip(jnp.exp(math.log(2.0) - 2.3025851 * jax.random.uniform(part_keys[4], (NZ, NX, NY), jnp.float32) ** level_of(part_keys[4], (NZ, NX, NY), ((0, 4), (1, 4)), -0.2, 0.2)), 0.2, 2.0)
    own_map = draw_own_map(jax.random.fold_in(jax.random.fold_in(key_of[12], part), 71), part)
    slot_table = plant(jax.random.randint(part_keys[6], (NZ // 2, NX // 2), 0, RX * RY), jax.random.fold_in(part_keys[6], 1), 0, (RX * RY) - 1).astype(jnp.int32)
    displacement = scatter_about(part_keys[7], (TX, TY, TZ), 1.0, 6.0, ((0, 4), (1, 4)), jnp.float32)
    displacement_prev = scatter_about(part_keys[8], (TX, TY, TZ), 1.0, 6.0, ((0, 4), (1, 4)), jnp.float32)
    layer_labels = plant(jax.random.randint(part_keys[9], (TX, TY, TZ), 0, LAYERS), jax.random.fold_in(part_keys[9], 1), 0, LAYERS - 1).astype(jnp.int32)
    shear_table = jnp.clip(jnp.exp(jax.random.uniform(part_keys[10], (LAYERS,), jnp.float32, math.log(0.05), math.log(0.15))), 0.05, 0.15)
    viscosity_table = jnp.clip(jnp.exp(jax.random.uniform(part_keys[11], (LAYERS,), jnp.float32, math.log(0.01), math.log(0.06))), 0.01, 0.06)
    return dict(pressure=pressure, pressure_prev=pressure_prev, courant=courant, nonlinearity=nonlinearity, absorption=absorption, own_map=own_map, slot_table=slot_table, displacement=displacement, displacement_prev=displacement_prev, layer_labels=layer_labels, shear_table=shear_table, viscosity_table=viscosity_table)


def laplace_pad(field):
    padded = jnp.pad(field, 1)
    total = padded[2:, 1:-1, 1:-1] + padded[:-2, 1:-1, 1:-1]
    total = total + padded[1:-1, 2:, 1:-1] + padded[1:-1, :-2, 1:-1]
    total = total + padded[1:-1, 1:-1, 2:] + padded[1:-1, 1:-1, :-2]
    return total - 6.0 * field

def acoustic_step(now, before, courant, nonlinearity, absorption):
    return 2.0 * now - before + courant * laplace_pad(now) + nonlinearity * (now * now - before * before) - 0.1 * absorption * (now - before)

def layer_lookup(labels, table):
    result = jnp.zeros(labels.shape, jnp.float32)
    for kind in range(table.shape[0]):
        result = result + jnp.where(labels == kind, table[kind], 0.0)
    return result

def reference(pressure, pressure_prev, courant, nonlinearity, absorption, own_map, slot_table, displacement, displacement_prev, layer_labels, shear_table, viscosity_table):
    pressure_mid = acoustic_step(pressure, pressure_prev, courant, nonlinearity, absorption)
    pressure_new = acoustic_step(pressure_mid, pressure, courant, nonlinearity, absorption)
    force = 0.1 * absorption * (pressure_mid * pressure_mid + pressure_new * pressure_new) * lax.rsqrt(courant)
    coarse = force.reshape(NZ // 2, 2, NX // 2, 2, TZ, 2).sum(axis=(1, 3, 5)) * 0.125
    rows = own_map // TCOLS * RX + slot_table // RY
    cols = own_map % TCOLS * RY + slot_table % RY
    target = jnp.where(own_map < TILES, rows * TY + cols, TX * TY).astype(jnp.int32)
    summed = jax.ops.segment_sum(coarse.reshape(-1, TZ), target.reshape(-1), num_segments=TX * TY + 1)
    tissue_force = summed[:-1].reshape(TX, TY, TZ)
    shear = layer_lookup(layer_labels, shear_table)
    viscosity = layer_lookup(layer_labels, viscosity_table)

    def elastic_step(now, before):
        return 2.0 * now - before + shear * laplace_pad(now) + viscosity * laplace_pad(now - before) + 0.25 * tissue_force
    displacement_mid = elastic_step(displacement, displacement_prev)
    displacement_new = elastic_step(displacement_mid, displacement)
    return (pressure_mid, pressure_new, tissue_force, displacement_mid, displacement_new)
```

```python
import functools

import jax
import jax.numpy as jnp
from jax import lax
from jax.experimental import pallas as pl
from jax.experimental.pallas import tpu as pltpu
from jax.sharding import PartitionSpec as P

MESH = pl.DeviceIdType.MESH
F32 = jnp.float32
BF16 = jnp.bfloat16


def iota(shape, dim):
    return lax.broadcasted_iota(jnp.int32, shape, dim)


def split(x):
    high = x.astype(BF16)
    low = (x - high.astype(F32)).astype(BF16)
    return high, low


def dot(a, b):
    return jnp.dot(a, b, preferred_element_type=F32)


def laplace(centre, up, down, left, right):
    rows, lanes = centre.shape
    row, lane = iota(centre.shape, 0), iota(centre.shape, 1)
    xm = jnp.where(row == 0, left, pltpu.roll(centre, 1, 0))
    xp = jnp.where(row == rows - 1, right, pltpu.roll(centre, rows - 1, 0))
    ym = jnp.where(lane == 0, 0.0, pltpu.roll(centre, 1, 1))
    yp = jnp.where(lane == lanes - 1, 0.0, pltpu.roll(centre, lanes - 1, 1))
    return ((up + down) + (xm + xp)) + ((ym + yp) - 6.0 * centre)


class Faces:
    def __init__(self, axis, first, last, halo, send, recv, base):
        size, index = lax.axis_size(axis), lax.axis_index(axis)
        self.halo = halo
        self.has_next, self.has_prev = index < size - 1, index > 0
        self.up = pltpu.make_async_remote_copy(
            src_ref=last, dst_ref=halo.at[0], send_sem=send.at[base], recv_sem=recv.at[base],
            device_id={axis: lax.rem(index + 1, size)}, device_id_type=MESH)
        self.down = pltpu.make_async_remote_copy(
            src_ref=first, dst_ref=halo.at[1], send_sem=send.at[base + 1], recv_sem=recv.at[base + 1],
            device_id={axis: lax.rem(index + size - 1, size)}, device_id_type=MESH)

    def clear(self):
        @pl.when(jnp.logical_not(self.has_prev))
        def _():
            self.halo[0] = jnp.zeros(self.halo.shape[1:], F32)

        @pl.when(jnp.logical_not(self.has_next))
        def _():
            self.halo[1] = jnp.zeros(self.halo.shape[1:], F32)

    def start(self):
        pl.when(self.has_next)(self.up.start)
        pl.when(self.has_prev)(self.down.start)

    def wait(self):
        pl.when(self.has_prev)(self.up.wait_recv)
        pl.when(self.has_next)(self.down.wait_recv)

    def wait_send(self):
        pl.when(self.has_next)(self.up.wait_send)
        pl.when(self.has_prev)(self.down.wait_send)


def kernel(
    capacity, slots,
    p_in, q_in, c_in, n_in, a_in, own, slot, u_in, w_in, k_in, shear_table, viscosity_table,
    pm, pn, tf, um, un,
    p, q, c, n, a, u, w, k, load,
    hz_p, hx_p, fx_p, hz_m, hx_m, fx_m,
    hz_u, hx_u, fx_u, hz_w, hx_w, fx_w, hz_e, hx_e, fx_e,
    rest, both, paired, packed, got, packed_places, got_places,
    send, recv, line_send, line_recv, place_send, place_recv,
):
    planes, rows, lateral = p.shape
    tile_rows, tile_cols, tile_depth = u.shape
    kinds = shear_table.shape[0]
    gx, gy = lax.axis_size("gx"), lax.axis_size("gy")
    blocks = gx * gy
    me = lax.axis_index("gx") * gy + lax.axis_index("gy")

    loads = [pltpu.make_async_copy(s, d, load.at[i]) for i, (s, d) in enumerate(
        ((p_in, p), (u_in, u), (w_in, w), (q_in, q), (c_in, c), (n_in, n), (a_in, a), (k_in, k)))]
    for copy in loads:
        copy.start()

    barrier = pltpu.get_barrier_semaphore()

    def greet(d, carry):
        other = lax.rem(me + d, blocks)
        pl.semaphore_signal(
            barrier, inc=1, device_id={"gx": other // gy, "gy": lax.rem(other, gy)}, device_id_type=MESH)
        return carry

    lax.fori_loop(1, blocks, greet, 0)

    def faces(first, last, halo, axis, base):
        return Faces(axis, first, last, halo, send, recv, base)

    def pair(field, hz, fx, hx, base):
        depth = field.shape[0]
        return (faces(field.at[0], field.at[depth - 1], hz, "gx", base),
                faces(fx.at[0], fx.at[1], hx, "gy", base + 2))

    p_z, p_x = pair(p, hz_p, fx_p, hx_p, 0)
    m_z, m_x = pair(pm, hz_m, fx_m, hx_m, 4)
    u_z, u_x = pair(u, hz_u, fx_u, hx_u, 8)
    w_z, w_x = pair(w, hz_w, fx_w, hx_w, 12)
    e_z, e_x = pair(um, hz_e, fx_e, hx_e, 16)
    every = (p_z, p_x, m_z, m_x, u_z, u_x, w_z, w_x, e_z, e_x)
    for item in every:
        item.clear()

    def stage(field, fx):
        def body(z, carry):
            plane = field[z]
            fx[0, pl.ds(z, 1), :] = plane[:1]
            fx[1, pl.ds(z, 1), :] = plane[-1:]
            return carry
        lax.fori_loop(0, field.shape[0], body, 0)

    loads[0].wait()
    stage(p, fx_p)
    pl.semaphore_wait(barrier, blocks - 1)
    p_z.start()
    p_x.start()
    loads[1].wait()
    loads[2].wait()
    stage(u, fx_u)
    stage(w, fx_w)
    u_z.start()
    u_x.start()
    w_z.start()
    w_x.start()

    lines_z, lines_x = own.shape
    count = lines_z * rows

    def along_lanes(table):
        column = iota((lines_z, count), 1)
        line_z, line_x = iota((lines_z, count), 0), lax.rem(column, rows) // 2
        here = line_z == column // rows
        total = jnp.zeros((lines_z, count), F32)
        for b in range(lines_x):
            total = total + jnp.where(here & (line_x == b), table[:, b:b + 1], 0.0)
        return jnp.sum(total, axis=0, keepdims=True)

    def along_rows(table):
        spread = jnp.concatenate(
            [jnp.broadcast_to(table[z:z + 1], (rows, lines_x)) for z in range(lines_z)], axis=0)
        row, line_x = iota((count, lines_x), 0), iota((count, lines_x), 1)
        return jnp.sum(jnp.where(line_x == lax.rem(row, rows) // 2, spread, 0.0), axis=1, keepdims=True)

    owners = own[...].astype(F32)
    owner_lane, owner_row = along_lanes(owners), along_rows(owners)
    place_lane = along_lanes(slot[...].astype(F32))
    earlier = iota((count, count), 0) // 2 < iota((count, count), 1) // 2
    rank = 0.5 * jnp.sum(
        jnp.where((owner_row == owner_lane) & earlier, 1.0, 0.0), axis=0, keepdims=True)
    target = owner_lane * float(slots) + rank
    match = iota((blocks * slots, count), 0).astype(F32) == target
    even = lax.rem(iota((blocks * slots, count), 1), 2) == 0
    places = jnp.sum(jnp.where(match & even, place_lane + 1.0, 0.0), axis=1, keepdims=True)
    packed_places[...] = jnp.broadcast_to(places, packed_places.shape)
    match = jnp.where(match, 1.0, 0.0).astype(BF16)

    def sends(source, target_ref, send_sems, recv_sems):
        def copy(d):
            other = lax.rem(me + d, blocks)
            return pltpu.make_async_remote_copy(
                src_ref=source.at[pl.ds(pl.multiple_of(other * slots, slots), slots)],
                dst_ref=target_ref.at[pl.ds(pl.multiple_of(me * slots, slots), slots)],
                send_sem=send_sems.at[d], recv_sem=recv_sems.at[d],
                device_id={"gx": other // gy, "gy": lax.rem(other, gy)}, device_id_type=MESH)

        def start():
            lax.fori_loop(1, blocks, lambda d, carry: (copy(d).start(), carry)[1], 0)
            here = pl.ds(pl.multiple_of(me * slots, slots), slots)
            target_ref[here, :] = source[here, :]

        def wait():
            lax.fori_loop(1, blocks, lambda d, carry: (copy(d).wait_recv(), carry)[1], 0)

        def wait_send():
            lax.fori_loop(1, blocks, lambda d, carry: (copy(d).wait_send(), carry)[1], 0)

        return start, wait, wait_send

    start_places, wait_places, wait_places_send = sends(packed_places, got_places, place_send, place_recv)
    start_lines, wait_lines, wait_lines_send = sends(packed, got, line_send, line_recv)
    start_places()

    def wave(now, before, lap, z):
        return (2.0 * now - before + c[z] * lap + n[z] * (now * now - before * before)
                - 0.1 * a[z] * (now - before))

    def first(z, up, down):
        now = p[z]
        lap = laplace(now, up, down, hx_p[0, pl.ds(z, 1), :], hx_p[1, pl.ds(z, 1), :])
        mid = wave(now, q[z], lap, z)
        pm[z] = mid
        fx_m[0, pl.ds(z, 1), :] = mid[:1]
        fx_m[1, pl.ds(z, 1), :] = mid[-1:]

    for copy in loads[3:7]:
        copy.wait()
    p_z.wait()
    p_x.wait()
    first(0, hz_p[0], p[1])
    first(planes - 1, p[planes - 2], hz_p[1])
    m_z.start()
    lax.fori_loop(1, planes - 1, lambda z, carry: (first(z, p[z - 1], p[z + 1]), carry)[1], 0)
    m_x.start()

    loads[7].wait()
    for item in (u_z, u_x, w_z, w_x):
        item.wait()

    def elastic(z, u_up, u_down, w_up, w_down):
        now, before, kind = u[z], w[z], k[z]
        lap_u = laplace(now, u_up, u_down, hx_u[0, pl.ds(z, 1), :], hx_u[1, pl.ds(z, 1), :])
        lap_w = laplace(before, w_up, w_down, hx_w[0, pl.ds(z, 1), :], hx_w[1, pl.ds(z, 1), :])
        shear, viscosity = jnp.zeros(now.shape, F32), jnp.zeros(now.shape, F32)
        for i in range(kinds):
            shear = jnp.where(kind == i, shear_table[i], shear)
            viscosity = jnp.where(kind == i, viscosity_table[i], viscosity)
        um[z] = 2.0 * now - before + shear * lap_u + viscosity * (lap_u - lap_w)
        rest[z] = now + viscosity * lap_u
        both[z] = shear + viscosity

    elastic(0, hz_u[0], u[1], hz_w[0], w[1])
    elastic(tile_rows - 1, u[tile_rows - 2], hz_u[1], w[tile_rows - 2], hz_w[1])
    lax.fori_loop(1, tile_rows - 1, lambda z, carry: (
        elastic(z, u[z - 1], u[z + 1], w[z - 1], w[z + 1]), carry)[1], 0)

    def second(z, up, down):
        now = pm[z]
        lap = laplace(now, up, down, hx_m[0, pl.ds(z, 1), :], hx_m[1, pl.ds(z, 1), :])
        new = wave(now, p[z], lap, z)
        pn[z] = new
        return 0.1 * a[z] * (now * now + new * new) * lax.rsqrt(c[z])

    def pair_at(i):
        return pl.ds(pl.multiple_of(i * rows, rows), rows)

    m_z.wait()
    m_x.wait()
    paired[pair_at(0), :] = second(0, hz_m[0], pm[1]) + second(1, pm[0], pm[2])
    last = planes // 2 - 1
    paired[pair_at(last), :] = second(planes - 2, pm[planes - 3], pm[planes - 1]) + second(
        planes - 1, pm[planes - 2], hz_m[1])

    def two(i, carry):
        z = 2 * i
        paired[pair_at(i), :] = second(z, pm[z - 1], pm[z + 1]) + second(z + 1, pm[z], pm[z + 2])
        return carry

    lax.fori_loop(1, last, two, 0)

    width = 256
    half = width // 2
    lanes_two = jnp.where(iota((width, half), 0) // 2 == iota((width, half), 1), 0.125, 0.0).astype(BF16)
    for i in range(lateral // width):
        high, low = split(paired[:, i * width:(i + 1) * width])
        coarse = dot(high, lanes_two) + dot(low, lanes_two)
        high, low = split(coarse)
        packed[:, i * half:(i + 1) * half] = dot(match, high) + dot(match, low)
    start_lines()

    wait_places()
    spots = jnp.transpose(got_places[...])[:1] - 1.0
    cells = tile_rows * tile_cols
    landing = jnp.where(
        iota((cells, blocks * slots), 0).astype(F32) == spots, 1.0, 0.0).astype(BF16)
    wait_lines()
    high, low = split(got[...])
    chunk = 4 if tile_rows % 4 == 0 else 1
    for r in range(0, tile_rows, chunk):
        part = landing[r * tile_cols:(r + chunk) * tile_cols]
        force = (dot(part, high) + dot(part, low)).reshape(chunk, tile_cols, tile_depth)
        tf[r:r + chunk] = force
        mid = um[r:r + chunk] + 0.25 * force
        um[r:r + chunk] = mid
        for j in range(chunk):
            fx_e[0, r + j:r + j + 1, :] = mid[j, :1]
            fx_e[1, r + j:r + j + 1, :] = mid[j, -1:]
    e_z.start()
    e_x.start()
    e_z.wait()
    e_x.wait()

    def final(z, up, down):
        now = um[z]
        lap = laplace(now, up, down, hx_e[0, pl.ds(z, 1), :], hx_e[1, pl.ds(z, 1), :])
        un[z] = 2.0 * now - rest[z] + both[z] * lap + 0.25 * tf[z]

    final(0, hz_e[0], um[1])
    final(tile_rows - 1, um[tile_rows - 2], hz_e[1])
    lax.fori_loop(1, tile_rows - 1, lambda z, carry: (final(z, um[z - 1], um[z + 1]), carry)[1], 0)
    for item in every:
        item.wait_send()
    wait_places_send()
    wait_lines_send()


def local(pressure, pressure_prev, courant, nonlinearity, absorption, own_map, slot_table,
          displacement, displacement_prev, layer_labels, shear_table, viscosity_table):
    planes, rows, lateral = pressure.shape
    tile = displacement.shape
    blocks = lax.axis_size("gx") * lax.axis_size("gy")
    capacity = max(2, own_map.shape[0] * own_map.shape[1] // blocks)
    slots = -(-capacity // 8) * 8
    anywhere = pl.BlockSpec(memory_space=pl.ANY)
    vmem = pl.BlockSpec(memory_space=pltpu.VMEM)
    smem = pl.BlockSpec(memory_space=pltpu.SMEM)
    wave, cell = pltpu.VMEM(pressure.shape, F32), pltpu.VMEM(tile, F32)

    def halos(shape):
        z, x = pltpu.VMEM((2,) + shape[1:], F32), pltpu.VMEM((2, shape[0], shape[2]), F32)
        return [z, x, x]

    dma = pltpu.SemaphoreType.DMA
    return pl.pallas_call(
        functools.partial(kernel, capacity, slots),
        out_shape=[jax.ShapeDtypeStruct(pressure.shape, F32)] * 2 + [jax.ShapeDtypeStruct(tile, F32)] * 3,
        in_specs=[anywhere] * 5 + [vmem] * 2 + [anywhere] * 3 + [smem] * 2,
        out_specs=[vmem] * 5,
        scratch_shapes=[wave] * 5 + [cell] * 2 + [pltpu.VMEM(tile, jnp.int32), dma((8,))]
        + halos(pressure.shape) * 2 + halos(tile) * 3
        + [cell, cell,
           pltpu.VMEM((planes // 2 * rows, lateral), F32),
           pltpu.VMEM((blocks * slots, lateral // 2), F32),
           pltpu.VMEM((blocks * slots, lateral // 2), F32),
           pltpu.VMEM((blocks * slots, 128), F32),
           pltpu.VMEM((blocks * slots, 128), F32),
           dma((20,)), dma((20,)), dma((blocks,)), dma((blocks,)), dma((blocks,)), dma((blocks,))],
        compiler_params=pltpu.CompilerParams(
            collective_id=0, has_side_effects=True, vmem_limit_bytes=40 * 1024 * 1024),
    )(pressure, pressure_prev, courant, nonlinearity, absorption, own_map, slot_table,
      displacement, displacement_prev, layer_labels, shear_table, viscosity_table)


def solution(mesh):
    field = P(("group", "gx"), "gy", None)
    table = P(("group", "gx"), "gy")
    return jax.shard_map(
        local,
        mesh=mesh,
        in_specs=(field,) * 5 + (table,) * 2 + (field,) * 3 + (P("group"),) * 2,
        out_specs=(field,) * 5,
        check_vma=False,
    )
```

```python
import functools

import jax
import jax.numpy as jnp
from jax import lax
from jax.experimental import pallas as pl
from jax.experimental.pallas import tpu as pltpu
from jax.sharding import PartitionSpec as P

MESH = pl.DeviceIdType.MESH
F32 = jnp.float32
BF16 = jnp.bfloat16


def iota(shape, dim):
    return lax.broadcasted_iota(jnp.int32, shape, dim)


def split(x):
    high = x.astype(BF16)
    low = (x - high.astype(F32)).astype(BF16)
    return high, low


def dot(a, b):
    return jnp.dot(a, b, preferred_element_type=F32)


def laplace(centre, up, down, left, right):
    rows, lanes = centre.shape
    row, lane = iota(centre.shape, 0), iota(centre.shape, 1)
    xm = jnp.where(row == 0, left, pltpu.roll(centre, 1, 0))
    xp = jnp.where(row == rows - 1, right, pltpu.roll(centre, rows - 1, 0))
    ym = jnp.where(lane == 0, 0.0, pltpu.roll(centre, 1, 1))
    yp = jnp.where(lane == lanes - 1, 0.0, pltpu.roll(centre, lanes - 1, 1))
    return ((up + down) + (xm + xp)) + ((ym + yp) - 6.0 * centre)


class Faces:
    def __init__(self, axis, first, last, halo, send, recv, base):
        size, index = lax.axis_size(axis), lax.axis_index(axis)
        self.halo = halo
        self.has_next, self.has_prev = index < size - 1, index > 0
        self.up = pltpu.make_async_remote_copy(
            src_ref=last, dst_ref=halo.at[0], send_sem=send.at[base], recv_sem=recv.at[base],
            device_id={axis: lax.rem(index + 1, size)}, device_id_type=MESH)
        self.down = pltpu.make_async_remote_copy(
            src_ref=first, dst_ref=halo.at[1], send_sem=send.at[base + 1], recv_sem=recv.at[base + 1],
            device_id={axis: lax.rem(index + size - 1, size)}, device_id_type=MESH)

    def clear(self):
        @pl.when(jnp.logical_not(self.has_prev))
        def _():
            self.halo[0] = jnp.zeros(self.halo.shape[1:], F32)

        @pl.when(jnp.logical_not(self.has_next))
        def _():
            self.halo[1] = jnp.zeros(self.halo.shape[1:], F32)

    def start(self):
        pl.when(self.has_next)(self.up.start)
        pl.when(self.has_prev)(self.down.start)

    def wait(self):
        pl.when(self.has_prev)(self.up.wait_recv)
        pl.when(self.has_next)(self.down.wait_recv)

    def wait_send(self):
        pl.when(self.has_next)(self.up.wait_send)
        pl.when(self.has_prev)(self.down.wait_send)


def kernel(
    capacity, slots,
    p_in, q_in, c_in, n_in, a_in, own_in, slot_in, u_in, w_in, k_in, shear_in, viscosity_in,
    pm, pn, tf, um, rest, both, hz_out, hx_out,
    p, q, c, n, a, u, w, k, own, slot, shear_table, viscosity_table, load,
    hz_p, hx_p, fx_p, hz_m, hx_m, fx_m,
    hz_u, hx_u, fx_u, hz_w, hx_w, fx_w, hz_e, hx_e, fx_e,
    paired, packed, got, packed_places, got_places,
    send, recv, line_send, line_recv, place_send, place_recv,
):
    planes, rows, lateral = p.shape
    tile_rows, tile_cols, tile_depth = u.shape
    kinds = shear_table.shape[0]
    gx, gy = lax.axis_size("gx"), lax.axis_size("gy")
    blocks = gx * gy
    me = lax.axis_index("gx") * gy + lax.axis_index("gy")

    loads = [pltpu.make_async_copy(s, d, load.at[i]) for i, (s, d) in enumerate(
        ((p_in, p), (u_in, u), (w_in, w), (own_in, own), (slot_in, slot), (shear_in, shear_table),
         (viscosity_in, viscosity_table), (q_in, q), (c_in, c), (n_in, n), (a_in, a), (k_in, k)))]
    for copy in loads:
        copy.start()

    barrier = pltpu.get_barrier_semaphore()

    def greet(d, carry):
        other = lax.rem(me + d, blocks)
        pl.semaphore_signal(
            barrier, inc=1, device_id={"gx": other // gy, "gy": lax.rem(other, gy)}, device_id_type=MESH)
        return carry

    lax.fori_loop(1, blocks, greet, 0)

    def faces(first, last, halo, axis, base):
        return Faces(axis, first, last, halo, send, recv, base)

    def pair(field, hz, fx, hx, base):
        depth = field.shape[0]
        return (faces(field.at[0], field.at[depth - 1], hz, "gx", base),
                faces(fx.at[0], fx.at[1], hx, "gy", base + 2))

    p_z, p_x = pair(p, hz_p, fx_p, hx_p, 0)
    m_z, m_x = pair(pm, hz_m, fx_m, hx_m, 4)
    u_z, u_x = pair(u, hz_u, fx_u, hx_u, 8)
    w_z, w_x = pair(w, hz_w, fx_w, hx_w, 12)
    e_z, e_x = pair(um, hz_e, fx_e, hx_e, 16)
    every = (p_z, p_x, m_z, m_x, u_z, u_x, w_z, w_x, e_z, e_x)
    for item in every:
        item.clear()

    def stage(field, fx):
        def body(z, carry):
            plane = field[z]
            fx[0, pl.ds(z, 1), :] = plane[:1]
            fx[1, pl.ds(z, 1), :] = plane[-1:]
            return carry
        lax.fori_loop(0, field.shape[0], body, 0)

    loads[0].wait()
    stage(p, fx_p)
    pl.semaphore_wait(barrier, blocks - 1)
    p_z.start()
    p_x.start()
    loads[1].wait()
    loads[2].wait()
    stage(u, fx_u)
    stage(w, fx_w)
    u_z.start()
    u_x.start()
    w_z.start()
    w_x.start()

    loads[3].wait()
    loads[4].wait()

    lines_x, lines_z = own.shape
    count = lines_z * rows
    padded = -(-count // 128) * 128

    def along_lanes(table):
        column = iota((lines_x, padded), 1)
        here = lax.rem(column, rows) // 2 == iota((lines_x, padded), 0)
        total = jnp.zeros((lines_x, padded), F32)
        for z in range(lines_z):
            total = total + jnp.where(here & (column // rows == z), table[:, z:z + 1], 0.0)
        return jnp.sum(total, axis=0, keepdims=True)

    owners = own[...].astype(F32)
    owner_lane = along_lanes(owners)
    owner_row = jnp.transpose(jnp.broadcast_to(owner_lane, (128, padded)))[:count, :1]
    owner_lane = owner_lane[:, :count]
    place_lane = along_lanes(slot[...].astype(F32))[:, :count]
    earlier = iota((count, count), 0) // 2 < iota((count, count), 1) // 2
    rank = 0.5 * jnp.sum(
        jnp.where((owner_row == owner_lane) & earlier, 1.0, 0.0), axis=0, keepdims=True)
    target = owner_lane * float(slots) + rank
    match = iota((blocks * slots, count), 0).astype(F32) == target
    even = lax.rem(iota((blocks * slots, count), 1), 2) == 0
    places = jnp.sum(jnp.where(match & even, place_lane + 1.0, 0.0), axis=1, keepdims=True)
    packed_places[...] = jnp.broadcast_to(places, packed_places.shape)
    match = jnp.where(match, 1.0, 0.0).astype(BF16)

    def sends(source, target_ref, send_sems, recv_sems):
        def copy(d):
            other = lax.rem(me + d, blocks)
            return pltpu.make_async_remote_copy(
                src_ref=source.at[pl.ds(pl.multiple_of(other * slots, slots), slots)],
                dst_ref=target_ref.at[pl.ds(pl.multiple_of(me * slots, slots), slots)],
                send_sem=send_sems.at[d], recv_sem=recv_sems.at[d],
                device_id={"gx": other // gy, "gy": lax.rem(other, gy)}, device_id_type=MESH)

        def start():
            lax.fori_loop(1, blocks, lambda d, carry: (copy(d).start(), carry)[1], 0)
            here = pl.ds(pl.multiple_of(me * slots, slots), slots)
            target_ref[here, :] = source[here, :]

        def wait():
            lax.fori_loop(1, blocks, lambda d, carry: (copy(d).wait_recv(), carry)[1], 0)

        def wait_send():
            lax.fori_loop(1, blocks, lambda d, carry: (copy(d).wait_send(), carry)[1], 0)

        return start, wait, wait_send

    start_places, wait_places, wait_places_send = sends(packed_places, got_places, place_send, place_recv)
    start_lines, wait_lines, wait_lines_send = sends(packed, got, line_send, line_recv)
    start_places()

    def wave(now, before, lap, z):
        return (2.0 * now - before + c[z] * lap + n[z] * (now * now - before * before)
                - 0.1 * a[z] * (now - before))

    def first(z, up, down):
        now = p[z]
        lap = laplace(now, up, down, hx_p[0, pl.ds(z, 1), :], hx_p[1, pl.ds(z, 1), :])
        mid = wave(now, q[z], lap, z)
        pm[z] = mid
        fx_m[0, pl.ds(z, 1), :] = mid[:1]
        fx_m[1, pl.ds(z, 1), :] = mid[-1:]

    for copy in loads[7:11]:
        copy.wait()
    p_z.wait()
    p_x.wait()
    first(0, hz_p[0], p[1])
    first(planes - 1, p[planes - 2], hz_p[1])
    m_z.start()
    lax.fori_loop(1, planes - 1, lambda z, carry: (first(z, p[z - 1], p[z + 1]), carry)[1], 0)
    m_x.start()

    loads[5].wait()
    loads[6].wait()
    loads[11].wait()
    for item in (u_z, u_x, w_z, w_x):
        item.wait()

    def elastic(z, u_up, u_down, w_up, w_down):
        now, before, kind = u[z], w[z], k[z]
        lap_u = laplace(now, u_up, u_down, hx_u[0, pl.ds(z, 1), :], hx_u[1, pl.ds(z, 1), :])
        lap_w = laplace(before, w_up, w_down, hx_w[0, pl.ds(z, 1), :], hx_w[1, pl.ds(z, 1), :])
        shear, viscosity = jnp.zeros(now.shape, F32), jnp.zeros(now.shape, F32)
        for i in range(kinds):
            shear = jnp.where(kind == i, shear_table[i], shear)
            viscosity = jnp.where(kind == i, viscosity_table[i], viscosity)
        um[z] = 2.0 * now - before + shear * lap_u + viscosity * (lap_u - lap_w)
        rest[z] = now + viscosity * lap_u
        both[z] = shear + viscosity

    elastic(0, hz_u[0], u[1], hz_w[0], w[1])
    elastic(tile_rows - 1, u[tile_rows - 2], hz_u[1], w[tile_rows - 2], hz_w[1])
    lax.fori_loop(1, tile_rows - 1, lambda z, carry: (
        elastic(z, u[z - 1], u[z + 1], w[z - 1], w[z + 1]), carry)[1], 0)

    def second(z, up, down):
        now = pm[z]
        lap = laplace(now, up, down, hx_m[0, pl.ds(z, 1), :], hx_m[1, pl.ds(z, 1), :])
        new = wave(now, p[z], lap, z)
        pn[z] = new
        return 0.1 * a[z] * (now * now + new * new) * lax.rsqrt(c[z])

    def pair_at(i):
        return pl.ds(pl.multiple_of(i * rows, rows), rows)

    m_z.wait()
    m_x.wait()
    paired[pair_at(0), :] = second(0, hz_m[0], pm[1]) + second(1, pm[0], pm[2])
    last = planes // 2 - 1
    paired[pair_at(last), :] = second(planes - 2, pm[planes - 3], pm[planes - 1]) + second(
        planes - 1, pm[planes - 2], hz_m[1])

    def two(i, carry):
        z = 2 * i
        paired[pair_at(i), :] = second(z, pm[z - 1], pm[z + 1]) + second(z + 1, pm[z], pm[z + 2])
        return carry

    lax.fori_loop(1, last, two, 0)

    width = 256
    half = width // 2
    lanes_two = jnp.where(iota((width, half), 0) // 2 == iota((width, half), 1), 0.125, 0.0).astype(BF16)
    for i in range(lateral // width):
        high, low = split(paired[:, i * width:(i + 1) * width])
        coarse = dot(high, lanes_two) + dot(low, lanes_two)
        high, low = split(coarse)
        packed[:, i * half:(i + 1) * half] = dot(match, high) + dot(match, low)
    start_lines()

    wait_places()
    spots = jnp.transpose(got_places[...])[:1] - 1.0
    cells = tile_rows * tile_cols
    landing = jnp.where(
        iota((cells, blocks * slots), 0).astype(F32) == spots, 1.0, 0.0).astype(BF16)
    wait_lines()
    high, low = split(got[...])
    chunk = 4 if tile_rows % 4 == 0 else 1
    for r in range(0, tile_rows, chunk):
        part = landing[r * tile_cols:(r + chunk) * tile_cols]
        force = (dot(part, high) + dot(part, low)).reshape(chunk, tile_cols, tile_depth)
        tf[r:r + chunk] = force
        mid = um[r:r + chunk] + 0.25 * force
        um[r:r + chunk] = mid
        for j in range(chunk):
            fx_e[0, r + j:r + j + 1, :] = mid[j, :1]
            fx_e[1, r + j:r + j + 1, :] = mid[j, -1:]
    e_z.start()
    e_x.start()
    e_z.wait()
    e_x.wait()

    hz_out[...] = hz_e[...]
    hx_out[...] = hx_e[...]
    for item in every:
        item.wait_send()
    wait_places_send()
    wait_lines_send()


def finish(pm, pn, tf, um, rest, both, hz, hx, pm_out, pn_out, tf_out, um_out, un_out, un, sems):
    copies = [pltpu.make_async_copy(s, d, sems.at[i]) for i, (s, d) in enumerate(
        ((pm, pm_out), (pn, pn_out), (tf, tf_out), (um, um_out)))]
    for copy in copies:
        copy.start()
    tile_rows = um.shape[0]

    def final(z, up, down):
        now = um[z]
        lap = laplace(now, up, down, hx[0, pl.ds(z, 1), :], hx[1, pl.ds(z, 1), :])
        un[z] = 2.0 * now - rest[z] + both[z] * lap + 0.25 * tf[z]

    final(0, hz[0], um[1])
    final(tile_rows - 1, um[tile_rows - 2], hz[1])
    lax.fori_loop(1, tile_rows - 1, lambda z, carry: (final(z, um[z - 1], um[z + 1]), carry)[1], 0)
    copies.append(pltpu.make_async_copy(un, un_out, sems.at[4]))
    copies[4].start()
    for copy in copies:
        copy.wait()


def local(pressure, pressure_prev, courant, nonlinearity, absorption, own_map, slot_table,
          displacement, displacement_prev, layer_labels, shear_table, viscosity_table):
    planes, rows, lateral = pressure.shape
    tile = displacement.shape
    blocks = lax.axis_size("gx") * lax.axis_size("gy")
    capacity = max(2, own_map.shape[0] * own_map.shape[1] // blocks)
    slots = -(-capacity // 8) * 8
    hbm = pl.BlockSpec(memory_space=pltpu.HBM)
    vmem = pl.BlockSpec(memory_space=pltpu.VMEM)
    wave, cell = pltpu.VMEM(pressure.shape, F32), pltpu.VMEM(tile, F32)

    def halos(shape):
        z, x = pltpu.VMEM((2,) + shape[1:], F32), pltpu.VMEM((2, shape[0], shape[2]), F32)
        return [z, x, x]

    dma = pltpu.SemaphoreType.DMA
    kinds = shear_table.shape[0]
    lines = pltpu.VMEM(own_map.shape[::-1], jnp.int32)
    waves = [jax.ShapeDtypeStruct(pressure.shape, F32)] * 2
    cells = [jax.ShapeDtypeStruct(tile, F32)]
    parts = pl.pallas_call(
        functools.partial(kernel, capacity, slots),
        out_shape=[wave] * 2 + [cell] * 4 + [pltpu.VMEM((2,) + tile[1:], F32),
                                             pltpu.VMEM((2, tile[0], tile[2]), F32)],
        in_specs=[hbm] * 12,
        out_specs=[vmem] * 8,
        scratch_shapes=[wave] * 5 + [cell] * 2 + [
            pltpu.VMEM(tile, jnp.int32), lines, lines,
            pltpu.SMEM((kinds,), F32), pltpu.SMEM((kinds,), F32), dma((12,))]
        + halos(pressure.shape) * 2 + halos(tile) * 3
        + [pltpu.VMEM((planes // 2 * rows, lateral), F32),
           pltpu.VMEM((blocks * slots, lateral // 2), F32),
           pltpu.VMEM((blocks * slots, lateral // 2), F32),
           pltpu.VMEM((blocks * slots, 128), F32),
           pltpu.VMEM((blocks * slots, 128), F32),
           dma((20,)), dma((20,)), dma((blocks,)), dma((blocks,)), dma((blocks,)), dma((blocks,))],
        compiler_params=pltpu.CompilerParams(
            collective_id=0, has_side_effects=True, vmem_limit_bytes=58 * 1024 * 1024),
    )(pressure, pressure_prev, courant, nonlinearity, absorption, own_map.T, slot_table.T,
      displacement, displacement_prev, layer_labels, shear_table, viscosity_table)
    return pl.pallas_call(
        finish,
        out_shape=waves + cells * 3,
        in_specs=[vmem] * 8,
        out_specs=[hbm] * 5,
        scratch_shapes=[cell, dma((5,))],
        compiler_params=pltpu.CompilerParams(vmem_limit_bytes=40 * 1024 * 1024),
    )(*parts)


def solution(mesh):
    field = P(("group", "gx"), "gy", None)
    table = P(("group", "gx"), "gy")
    return jax.shard_map(
        local,
        mesh=mesh,
        in_specs=(field,) * 5 + (table,) * 2 + (field,) * 3 + (P("group"),) * 2,
        out_specs=(field,) * 5,
        check_vma=False,
    )
```
